16 devices in a mesh: rep: 2 (over y, z), dp: 8 (over x, core).
Axes of the slice: x: 4, y: 2, z: 1, core: 2. Of those that a mesh axis runs over, the one named last changes fastest.
The devices are a block of a 4x4x8 slice.
Arguments:
- x: bfloat16 [16, 2048, 768], P(('rep', 'dp')), parts along dimension 0
- dy: bfloat16 [16, 2048, 768], P(('rep', 'dp')), parts along dimension 0
- w_gate: bfloat16 [2, 768, 2304], replicated
- w_up: bfloat16 [2, 768, 2304], replicated
- w_down: bfloat16 [2, 2304, 768], replicated
- m_w_gate: float32 [2, 768, 2304], replicated
- m_w_up: float32 [2, 768, 2304], replicated
- m_w_down: float32 [2, 2304, 768], replicated
- v_w_gate: float32 [2, 768, 2304], replicated
- v_w_up: float32 [2, 768, 2304], replicated
- v_w_down: float32 [2, 2304, 768], replicated
Outputs:
- output 1: bfloat16 [4, 768, 2304], P('rep'), parts along dimension 0
- output 2: bfloat16 [4, 768, 2304], P('rep'), parts along dimension 0
- output 3: bfloat16 [4, 2304, 768], P('rep'), parts along dimension 0
- output 4: float32 [4, 768, 2304], P('rep'), parts along dimension 0
- output 5: float32 [4, 768, 2304], P('rep'), parts along dimension 0
- output 6: float32 [4, 2304, 768], P('rep'), parts along dimension 0
- output 7: float32 [4, 768, 2304], P('rep'), parts along dimension 0
- output 8: float32 [4, 768, 2304], P('rep'), parts along dimension 0
- output 9: float32 [4, 2304, 768], P('rep'), parts along dimension 0
There are 2 independent parts. The reference program is written for one: setup_inputs(seed, part) draws one part's arguments, and reference() takes and returns one part's arrays. A program takes and returns all parts, laid end to end along the dimension named above; an argument that names none is the same for every part.
All inputs are finite; a program needn't handle non-finite values.
Results may differ from the reference program's by a relative error of at most 0.022.
Values are sent between devices in bfloat16 or wider.
A program may use at most 768 MiB of HBM per device.

```python
import jax
import jax.numpy as jnp
from jax import lax

SEQUENCES = 8
TOKENS = 2048
D = 768
FF = 2304
LAYERS = 2
NAMES = ("w_gate", "w_up", "w_down")
SHAPES = {"w_gate": (LAYERS, D, FF), "w_up": (LAYERS, D, FF), "w_down": (LAYERS, FF, D)}


def bump(key, n, height):
    away = (jnp.arange(n, dtype=jnp.int32) - jax.random.randint(key, (), 0, n, jnp.int32)) % n
    return jnp.where(away < n // 8, height, 1.0)


def together(key, own, strength):
    shared = jax.random.normal(key, own.shape[1:], jnp.float32)
    return (own + strength * shared) * lax.rsqrt(1 + strength * strength)


def setup_inputs(seed: int = 0, part: int = 0) -> dict:
    kx, kdy, ka, kb, kz, kf, kh, kl, *keys = jax.random.split(jax.random.key(seed), 8 + 3 * len(NAMES))
    kx, kdy, ka, kb = (jax.random.fold_in(k, part) for k in (kx, kdy, ka, kb))
    kw, km, kv = (keys[i::3] for i in range(3))
    shape = (SEQUENCES, TOKENS, D)
    much_x, much_dy = jax.random.uniform(kz, (2,), jnp.float32, 0.0, 1.0)
    loud = 2.0 ** jax.random.uniform(jax.random.fold_in(kz, 1), (), jnp.float32, -1.0, 2.0)
    layers = 2.0 ** jax.random.uniform(kl, (LAYERS, 1, 1), jnp.float32, -1.0, 1.0)
    x = together(ka, jax.random.normal(kx, shape, jnp.float32), much_x) * bump(kf, D, 4.0)
    dy = together(kb, jax.random.normal(kdy, shape, jnp.float32), much_dy)
    drawn = {"x": x.astype(jnp.bfloat16), "dy": (loud * dy * (SEQUENCES * TOKENS) ** -0.5).astype(jnp.bfloat16)}
    for key, name in zip(kw, NAMES, strict=True):
        w = jax.random.normal(key, SHAPES[name], jnp.float32) * SHAPES[name][1] ** -0.5
        drawn[name] = (w * {"w_gate": 1.0, "w_up": bump(kh, FF, 4.0), "w_down": layers}[name]).astype(jnp.bfloat16)
    for key, name in zip(km, NAMES, strict=True):
        drawn[f"m_{name}"] = 0.1 * jax.random.normal(key, SHAPES[name], jnp.float32)
    for key, name in zip(kv, NAMES, strict=True):
        drawn[f"v_{name}"] = jax.random.uniform(key, SHAPES[name], jnp.float32, 0.005, 0.015)
    return drawn


def matmul(a, w):
    return jnp.dot(a, w, preferred_element_type=jnp.float32).astype(jnp.bfloat16)


def normed(h):
    wide = h.astype(jnp.float32)
    scale = lax.rsqrt(jnp.mean(wide**2, -1, keepdims=True) + 1e-6)
    return (wide * scale).astype(jnp.bfloat16)


def layer(h, w):
    a = normed(h)
    gate = jnp.dot(a, w["w_gate"], preferred_element_type=jnp.float32)
    up = jnp.dot(a, w["w_up"], preferred_element_type=jnp.float32)
    return h + matmul((jax.nn.silu(gate) * up).astype(jnp.bfloat16), w["w_down"])


def adamw(w, m, v, g):
    m = 0.9 * m + 0.1 * g
    v = 0.95 * v + 0.05 * g * g
    step = m * lax.rsqrt(v + 1e-8) + 0.1 * w
    return (w - 0.02 * step).astype(jnp.bfloat16), m, v


def stack(weights, h):
    return lax.scan(lambda h, w: (layer(h, w), None), h, weights)[0]


def reference(x, dy, w_gate, w_up, w_down, m_w_gate, m_w_up, m_w_down, v_w_gate, v_w_up, v_w_down):
    weights = dict(zip(NAMES, (w_gate, w_up, w_down), strict=True))

    def take(so_far, sequence):
        h, by_y = sequence
        _, back = jax.vjp(lambda w: stack(w, h), weights)
        return jax.tree.map(lambda total, term: total + term.astype(jnp.float32), so_far, back(by_y)[0]), None

    none_yet = {name: jnp.zeros(w.shape, jnp.float32) for name, w in weights.items()}
    by_weights, _ = lax.scan(take, none_yet, (x, dy))
    gradients = [by_weights[name].astype(jnp.bfloat16).astype(jnp.float32) for name in NAMES]
    new = [
        adamw(w.astype(jnp.float32), m, v, g)
        for w, m, v, g in zip((w_gate, w_up, w_down), (m_w_gate, m_w_up, m_w_down), (v_w_gate, v_w_up, v_w_down), gradients, strict=True)
    ]
    return tuple(one[which] for which in range(3) for one in new)
```

```python
import functools

import jax
import jax.numpy as jnp
from jax import lax
from jax.experimental import pallas as pl
from jax.experimental.pallas import tpu as pltpu
from jax.sharding import PartitionSpec as P

BF16, F32 = jnp.bfloat16, jnp.float32
FB = 256
FB_FWD = 768
TT = 512
VMEM = 60 * 2**20


def dot(a, b):
    return jnp.dot(a, b, preferred_element_type=F32)


def dot_nt(a, b):
    return lax.dot_general(a, b, (((1,), (1,)), ((), ())), preferred_element_type=F32)


def transposed(eye, x):
    return dot_nt(eye, x).astype(BF16)


def scale_of(wide):
    return lax.rsqrt(jnp.mean(wide * wide, -1, keepdims=True) + 1e-6)


def sigmoid(x):
    return 1.0 / (1.0 + jnp.exp(-x))


def forward_kernel(h_ref, wg_ref, wu_ref, wd_ref, out_ref, a_ref, acc_ref):
    step, steps = pl.program_id(0), pl.num_programs(0)
    tokens = h_ref.shape[0]

    @pl.when(step == 0)
    def _():
        def tile(i, _):
            rows = pl.ds(i * TT, TT)
            wide = h_ref[rows, :].astype(F32)
            a_ref[rows, :] = (wide * scale_of(wide)).astype(BF16)
            acc_ref[rows, :] = jnp.zeros((TT, acc_ref.shape[1]), F32)
            return 0

        lax.fori_loop(0, tokens // TT, tile, 0)

    def tile(i, _):
        rows = pl.ds(i * TT, TT)
        a = a_ref[rows, :]
        gate = dot(a, wg_ref[0])
        up = dot(a, wu_ref[0])
        hid = (gate * sigmoid(gate) * up).astype(BF16)
        acc_ref[rows, :] += dot(hid, wd_ref[0])
        return 0

    lax.fori_loop(0, tokens // TT, tile, 0)

    @pl.when(step == steps - 1)
    def _():
        def tile(i, _):
            rows = pl.ds(i * TT, TT)
            down = acc_ref[rows, :].astype(BF16).astype(F32)
            out_ref[rows, :] = (h_ref[rows, :].astype(F32) + down).astype(BF16)
            return 0

        lax.fori_loop(0, tokens // TT, tile, 0)


def forward(h, weights, number):
    tokens, d = h.shape
    ff = weights[0].shape[2]
    return pl.pallas_call(
        forward_kernel,
        grid=(ff // FB_FWD,),
        in_specs=[
            pl.BlockSpec((tokens, d), lambda f: (0, 0), pipeline_mode=pl.Buffered(1)),
            pl.BlockSpec((1, d, FB_FWD), lambda f: (number, 0, f)),
            pl.BlockSpec((1, d, FB_FWD), lambda f: (number, 0, f)),
            pl.BlockSpec((1, FB_FWD, d), lambda f: (number, f, 0)),
        ],
        out_specs=pl.BlockSpec((tokens, d), lambda f: (0, 0), pipeline_mode=pl.Buffered(1)),
        out_shape=jax.ShapeDtypeStruct((tokens, d), BF16),
        scratch_shapes=[pltpu.VMEM((tokens, d), BF16), pltpu.VMEM((tokens, d), F32)],
        compiler_params=pltpu.CompilerParams(vmem_limit_bytes=VMEM, dimension_semantics=("arbitrary",)),
        cost_estimate=pl.CostEstimate(flops=6 * tokens * d * ff, bytes_accessed=4 * tokens * d + 6 * d * ff, transcendentals=tokens * ff),
        name="layer_forward",
    )(h, *weights)


SLOTS = 4
MESH = pl.DeviceIdType.MESH


def backward_kernel(with_input, n, h_ref, g_ref, wg_ref, wu_ref, wd_ref, *refs):
    if with_input:
        shard_ref, dh_ref, *refs, acc_ref = refs
    else:
        shard_ref, *refs = refs
    a_ref, at_ref, gt_ref, hid_ref, dgate_ref, dup_ref, own, recv_a, send_b, recv_b, send_c, recv_c, *sems = refs
    send_a_sem, recv_a_sem, send_b_sem, recv_b_sem, send_c_sem, recv_c_sem = sems
    step, blocks = pl.program_id(0), pl.num_programs(0) - SLOTS
    tokens, d = h_ref.shape
    share, half = own.shape[3], own.shape[3] // 2
    chips = n // 2
    me = lax.axis_index("dp")
    chip, core = lax.div(me, 2), lax.rem(me, 2)
    right_chip, far_chip, left_chip = (lax.rem(chip + i, chips) for i in (1, 2, 3))
    partner = chip * 2 + (1 - core)
    sides = (right_chip * 2 + core, left_chip * 2 + core)

    def copy_a(block):
        slot = lax.rem(block, SLOTS)
        return pltpu.make_async_remote_copy(
            own.at[slot, 1 - core], recv_a.at[slot], send_a_sem.at[slot], recv_a_sem.at[slot], device_id={"dp": partner}, device_id_type=MESH
        )

    def copy_b(block, way):
        slot = lax.rem(block, SLOTS)
        return pltpu.make_async_remote_copy(
            send_b.at[slot, way],
            recv_b.at[slot, way],
            send_b_sem.at[slot, way],
            recv_b_sem.at[slot, way],
            device_id={"dp": sides[way]},
            device_id_type=MESH,
        )

    def copy_c(block, way):
        slot = lax.rem(block, SLOTS)
        return pltpu.make_async_remote_copy(
            send_c.at[slot, way],
            recv_c.at[slot, way],
            send_c_sem.at[slot, way],
            recv_c_sem.at[slot, way],
            device_id={"dp": sides[way]},
            device_id_type=MESH,
        )

    def on_chip(slot, which, rows):
        return own[slot, core, which, rows].astype(F32) + recv_a[slot, which, rows].astype(F32)

    @pl.when(step == 0)
    def _():
        barrier = pltpu.get_barrier_semaphore()
        for other in (partner, *sides):
            pl.semaphore_signal(barrier, inc=1, device_id={"dp": other}, device_id_type=MESH)

    @pl.when(step == 1)
    def _():
        pl.semaphore_wait(pltpu.get_barrier_semaphore(), 3)

    first, second = pl.ds(0, half), pl.ds(half, half)

    @pl.when(step >= 4)
    def _():
        block = step - 4
        slot = lax.rem(block, SLOTS)
        copy_c(block, 0).wait()
        copy_c(block, 1).wait()
        for rows in (first, second):
            total = on_chip(slot, chip, rows) + recv_c[slot, 0, rows].astype(F32) + recv_c[slot, 1, rows].astype(F32)
            shard_ref[0, rows] = total.astype(BF16)

    @pl.when((step >= 3) & (step < blocks + 3))
    def _():
        block = step - 3
        slot = lax.rem(block, SLOTS)
        copy_b(block, 0).wait()
        copy_b(block, 1).wait()
        send_c[slot, 0, first] = (on_chip(slot, right_chip, first) + recv_b[slot, 0].astype(F32)).astype(BF16)
        send_c[slot, 0, second] = on_chip(slot, right_chip, second).astype(BF16)
        send_c[slot, 1, first] = on_chip(slot, left_chip, first).astype(BF16)
        send_c[slot, 1, second] = (on_chip(slot, left_chip, second) + recv_b[slot, 1].astype(F32)).astype(BF16)
        copy_c(block, 0).start()
        copy_c(block, 1).start()

    @pl.when((step >= 2) & (step < blocks + 2))
    def _():
        block = step - 2
        slot = lax.rem(block, SLOTS)
        copy_a(block).wait()
        send_b[slot, 0] = on_chip(slot, far_chip, first).astype(BF16)
        send_b[slot, 1] = on_chip(slot, far_chip, second).astype(BF16)
        copy_b(block, 0).start()
        copy_b(block, 1).start()

    @pl.when((step >= 1) & (step < blocks + 1))
    def _():
        copy_a(step - 1).start()

    eye = (lax.broadcasted_iota(jnp.int32, (FB, FB), 0) == lax.broadcasted_iota(jnp.int32, (FB, FB), 1)).astype(BF16)

    @pl.when(step == 0)
    def _():
        def tile(i, _):
            rows = pl.ds(pl.multiple_of(i * TT, TT), TT)
            wide = h_ref[rows, :].astype(F32)
            a_ref[rows, :] = (wide * scale_of(wide)).astype(BF16)
            for j in range(d // FB):
                at_ref[j * FB : (j + 1) * FB, rows] = transposed(eye, a_ref[rows, j * FB : (j + 1) * FB])
                gt_ref[j * FB : (j + 1) * FB, rows] = transposed(eye, g_ref[rows, j * FB : (j + 1) * FB])
            if with_input:
                acc_ref[rows, :] = jnp.zeros((TT, d), F32)
            return 0

        lax.fori_loop(0, tokens // TT, tile, 0)

    @pl.when(step < blocks)
    def _():
        slot = lax.rem(step, SLOTS)
        wg, wu, wd = wg_ref[0], wu_ref[0], wd_ref[0]
        for i in range(tokens // TT):
            rows = pl.ds(i * TT, TT)
            a = a_ref[rows, :]
            gate, up = dot(a, wg), dot(a, wu)
            dhid = dot_nt(g_ref[rows, :], wd).astype(BF16).astype(F32)
            sig = sigmoid(gate)
            silu = gate * sig
            hid_ref[rows, :] = (silu * up).astype(BF16)
            dup_ref[rows, :] = (dhid * silu).astype(BF16)
            dgate_ref[rows, :] = (dhid * up * (sig + silu * (1.0 - sig))).astype(BF16)
        part, down = d // n, FB // n
        for i in range(d // FB):
            rows = pl.ds(i * FB, FB)
            dwg = dot(at_ref[rows, :], dgate_ref[...]).astype(BF16)
            dwu = dot(at_ref[rows, :], dup_ref[...]).astype(BF16)
            dwd = transposed(eye, dot(gt_ref[rows, :], hid_ref[...]).astype(BF16))
            lo, hi = i * FB, (i + 1) * FB
            for k in range(n):
                top, end = max(lo, k * part), min(hi, (k + 1) * part)
                if top < end:
                    own[slot, k % 2, k // 2, top - k * part : end - k * part, :] = dwg[top - lo : end - lo]
                    own[slot, k % 2, k // 2, part + top - k * part : part + end - k * part, :] = dwu[top - lo : end - lo]
                own[slot, k % 2, k // 2, 2 * part + i * down : 2 * part + (i + 1) * down, :] = dwd[k * down : (k + 1) * down]
        if with_input:
            for i in range(tokens // TT):
                rows = pl.ds(i * TT, TT)
                acc_ref[rows, :] += dot_nt(dgate_ref[rows, :], wg) + dot_nt(dup_ref[rows, :], wu)

    if with_input:

        @pl.when(step == blocks)
        def _():
            def tile(i, _):
                rows = pl.ds(i * TT, TT)
                wide = h_ref[rows, :].astype(F32)
                scale = scale_of(wide)
                da = acc_ref[rows, :].astype(BF16).astype(F32)
                along = jnp.mean(da * wide, -1, keepdims=True)
                dwide = (da * scale - wide * (scale * scale * scale * along)).astype(BF16)
                dh_ref[rows, :] = (g_ref[rows, :].astype(F32) + dwide.astype(F32)).astype(BF16)
                return 0

            lax.fori_loop(0, tokens // TT, tile, 0)


def backward(h, g, weights, number, n, with_input):
    tokens, d = h.shape
    ff = weights[0].shape[2]
    blocks = ff // FB
    chips, share = n // 2, 3 * d // n
    assert chips == 4
    whole = pl.BlockSpec((tokens, d), lambda f: (0, 0), pipeline_mode=pl.Buffered(1))
    outs = [jax.ShapeDtypeStruct((blocks, share, FB), BF16)]
    out_specs = [pl.BlockSpec((1, share, FB), lambda f: (jnp.maximum(f - SLOTS, 0), 0, 0))]
    scratch = [pltpu.VMEM((tokens, d), BF16), pltpu.VMEM((d, tokens), BF16), pltpu.VMEM((d, tokens), BF16)]
    scratch += [pltpu.VMEM((tokens, FB), BF16)] * 3
    scratch += [
        pltpu.VMEM((SLOTS, 2, chips, share, FB), BF16),
        pltpu.VMEM((SLOTS, chips, share, FB), BF16),
        pltpu.VMEM((SLOTS, 2, share // 2, FB), BF16),
        pltpu.VMEM((SLOTS, 2, share // 2, FB), BF16),
        pltpu.VMEM((SLOTS, 2, share, FB), BF16),
        pltpu.VMEM((SLOTS, 2, share, FB), BF16),
    ]
    scratch += [pltpu.SemaphoreType.DMA((SLOTS,))] * 2 + [pltpu.SemaphoreType.DMA((SLOTS, 2))] * 4
    if with_input:
        outs.append(jax.ShapeDtypeStruct((tokens, d), BF16))
        out_specs.append(whole)
        scratch.append(pltpu.VMEM((tokens, d), F32))
    return pl.pallas_call(
        functools.partial(backward_kernel, with_input, n),
        grid=(blocks + SLOTS,),
        in_specs=[
            whole,
            whole,
            pl.BlockSpec((1, d, FB), lambda f: (number, 0, jnp.minimum(f, blocks - 1))),
            pl.BlockSpec((1, d, FB), lambda f: (number, 0, jnp.minimum(f, blocks - 1))),
            pl.BlockSpec((1, FB, d), lambda f: (number, jnp.minimum(f, blocks - 1), 0)),
        ],
        out_specs=out_specs,
        out_shape=outs,
        scratch_shapes=scratch,
        compiler_params=pltpu.CompilerParams(
            vmem_limit_bytes=VMEM, dimension_semantics=("arbitrary",), collective_id=number, has_side_effects=True
        ),
        cost_estimate=pl.CostEstimate(
            flops=(16 if with_input else 12) * tokens * d * ff, bytes_accessed=6 * tokens * d + 12 * d * ff, transcendentals=tokens * ff
        ),
        name=f"layer_backward_{number}",
    )(h, g, *weights)


def adamw_kernel(sum_ref, *refs):
    ws, ms, vs, outs = refs[:3], refs[3:6], refs[6:9], refs[-9:]
    share = sum_ref.shape[2] // 3
    some = sum_ref.shape[0]
    for i in range(3):
        if i < 2:
            g = sum_ref[:, 0, i * share : (i + 1) * share, :].reshape(some * share, FB)
        else:
            down = ws[2].shape[1] // some
            pieces = [
                sum_ref[:, 0, 2 * share + j * down : 2 * share + (j + 1) * down, :].reshape(some * down, FB) for j in range(share // down)
            ]
            g = jnp.concatenate(pieces, axis=1)
        g = g.astype(F32)
        w, m, v = ws[i][0].astype(F32), ms[i][0], vs[i][0]
        m = 0.9 * m + 0.1 * g
        v = 0.95 * v + 0.05 * g * g
        step = m * lax.rsqrt(v + 1e-8) + 0.1 * w
        outs[i][0] = (w - 0.02 * step).astype(BF16)
        outs[3 + i][0] = m
        outs[6 + i][0] = v


def adamw(sums, arrays, number, so_far):
    n, blocks, share, _ = sums.shape
    parts = 2
    d, ff = arrays[0].shape[1:]
    wide = pl.BlockSpec((1, d // parts, FB), lambda f, p: (number, p, f))
    tall = pl.BlockSpec((1, FB // parts, d), lambda f, p: (number, f * parts + p, 0))
    three = [wide, wide, tall]
    held = list(so_far) if so_far is not None else []
    return pl.pallas_call(
        adamw_kernel,
        grid=(blocks, parts),
        in_specs=[pl.BlockSpec((n // parts, 1, share, FB), lambda f, p: (p, f, 0, 0))] + three * 3 + [pl.BlockSpec(memory_space=pl.ANY)] * len(held),
        out_specs=three * 3,
        out_shape=[jax.ShapeDtypeStruct(a.shape, a.dtype) for a in arrays],
        input_output_aliases={10 + i: i for i in range(len(held))},
        compiler_params=pltpu.CompilerParams(vmem_limit_bytes=VMEM, dimension_semantics=("arbitrary", "arbitrary")),
        cost_estimate=pl.CostEstimate(flops=3 * 14 * d * ff, bytes_accessed=3 * 22 * d * ff, transcendentals=3 * d * ff),
        name=f"adamw_{number}",
    )(sums, *arrays, *held)


def solution(mesh):
    n = mesh.shape["dp"]

    def step(x, dy, *arrays):
        weights = arrays[:3]
        layers = weights[0].shape[0]
        h, kept = x[0], []
        for number in range(layers):
            kept.append(h)
            if number < layers - 1:
                h = forward(h, weights, number)
        g, sums = dy[0], [None] * layers
        for number in reversed(range(layers)):
            shard, *rest = backward(kept[number], g, weights, number, n, number > 0)
            if number < layers - 1:
                shard, sums[number + 1] = lax.optimization_barrier((shard, sums[number + 1]))
            sums[number] = lax.all_gather(shard, "dp")
            if rest:
                (g,) = rest
        new = None
        for number in reversed(range(layers)):
            new = adamw(sums[number], arrays, number, new)
        return tuple(new)

    return jax.shard_map(
        step,
        mesh=mesh,
        in_specs=(P(("rep", "dp"), None, None),) * 2 + (P(None, None, None),) * 9,
        out_specs=(P("rep", None, None),) * 9,
        check_vma=False,
    )
```

```python
import functools

import jax
import jax.numpy as jnp
from jax import lax
from jax.experimental import pallas as pl
from jax.experimental.pallas import tpu as pltpu
from jax.sharding import PartitionSpec as P

BF16, F32 = jnp.bfloat16, jnp.float32
FB = 256
FB_FWD = 768
TT = 512
VMEM = 60 * 2**20


def dot(a, b):
    return jnp.dot(a, b, preferred_element_type=F32)


def dot_nt(a, b):
    return lax.dot_general(a, b, (((1,), (1,)), ((), ())), preferred_element_type=F32)


def transposed(eye, x):
    return dot_nt(eye, x).astype(BF16)


def scale_of(wide):
    return lax.rsqrt(jnp.mean(wide * wide, -1, keepdims=True) + 1e-6)


def sigmoid(x):
    return 1.0 / (1.0 + jnp.exp(-x))


def forward_kernel(h_ref, wg_ref, wu_ref, wd_ref, out_ref, a_ref, acc_ref):
    step, steps = pl.program_id(0), pl.num_programs(0)
    tokens = h_ref.shape[0]

    @pl.when(step == 0)
    def _():
        def tile(i, _):
            rows = pl.ds(i * TT, TT)
            wide = h_ref[rows, :].astype(F32)
            a_ref[rows, :] = (wide * scale_of(wide)).astype(BF16)
            acc_ref[rows, :] = jnp.zeros((TT, acc_ref.shape[1]), F32)
            return 0

        lax.fori_loop(0, tokens // TT, tile, 0)

    def tile(i, _):
        rows = pl.ds(i * TT, TT)
        a = a_ref[rows, :]
        gate = dot(a, wg_ref[0])
        up = dot(a, wu_ref[0])
        hid = (gate * sigmoid(gate) * up).astype(BF16)
        acc_ref[rows, :] += dot(hid, wd_ref[0])
        return 0

    lax.fori_loop(0, tokens // TT, tile, 0)

    @pl.when(step == steps - 1)
    def _():
        def tile(i, _):
            rows = pl.ds(i * TT, TT)
            down = acc_ref[rows, :].astype(BF16).astype(F32)
            out_ref[rows, :] = (h_ref[rows, :].astype(F32) + down).astype(BF16)
            return 0

        lax.fori_loop(0, tokens // TT, tile, 0)


def forward(h, weights, number):
    tokens, d = h.shape
    ff = weights[0].shape[2]
    return pl.pallas_call(
        forward_kernel,
        grid=(ff // FB_FWD,),
        in_specs=[
            pl.BlockSpec((tokens, d), lambda f: (0, 0), pipeline_mode=pl.Buffered(1)),
            pl.BlockSpec((1, d, FB_FWD), lambda f: (number, 0, f)),
            pl.BlockSpec((1, d, FB_FWD), lambda f: (number, 0, f)),
            pl.BlockSpec((1, FB_FWD, d), lambda f: (number, f, 0)),
        ],
        out_specs=pl.BlockSpec((tokens, d), lambda f: (0, 0), pipeline_mode=pl.Buffered(1)),
        out_shape=jax.ShapeDtypeStruct((tokens, d), BF16),
        scratch_shapes=[pltpu.VMEM((tokens, d), BF16), pltpu.VMEM((tokens, d), F32)],
        compiler_params=pltpu.CompilerParams(vmem_limit_bytes=VMEM, dimension_semantics=("arbitrary",)),
        cost_estimate=pl.CostEstimate(flops=6 * tokens * d * ff, bytes_accessed=4 * tokens * d + 6 * d * ff, transcendentals=tokens * ff),
        name="layer_forward",
    )(h, *weights)


SLOTS, HELD = 4, 6
LATE = 5
MESH = pl.DeviceIdType.MESH


def backward_kernel(n, layers, late, *refs):
    kept, (dy_ref, wg_ref, wu_ref, wd_ref, sums_ref, late_ref), refs = refs[:layers], refs[layers : layers + 6], refs[layers + 6 :]
    g_ref, a_ref, at_ref, gt_ref, hid_ref, dgate_ref, dup_ref, acc_ref, *refs = refs
    own, recv_a, send_b, recv_b, send_c, recv_c, held, *sems = refs
    send_a_sem, recv_a_sem, send_b_sem, recv_b_sem, send_c_sem, recv_c_sem, send_g_sem, recv_g_sem, out_sem = sems
    step = pl.program_id(0)
    tokens, d = dy_ref.shape
    blocks = pl.num_programs(0) - SLOTS - 1
    each, early = blocks // layers, blocks - late
    share, half = own.shape[3], own.shape[3] // 2
    chips = n // 2
    me = lax.axis_index("dp")
    chip, core = lax.div(me, 2), lax.rem(me, 2)
    right_chip, far_chip, left_chip = (lax.rem(chip + i, chips) for i in (1, 2, 3))
    partner = chip * 2 + (1 - core)
    right, far, left = (c * 2 + core for c in (right_chip, far_chip, left_chip))
    sides = (right, left)
    first, second = pl.ds(0, half), pl.ds(half, half)

    def remote(src, dst, send, recv, other):
        return pltpu.make_async_remote_copy(src, dst, send, recv, device_id={"dp": other}, device_id_type=MESH)

    def copy_a(block):
        slot = lax.rem(block, SLOTS)
        return remote(own.at[slot, 1 - core], recv_a.at[slot], send_a_sem.at[slot], recv_a_sem.at[slot], partner)

    def copy_b(block, way):
        slot = lax.rem(block, SLOTS)
        return remote(send_b.at[slot, way], recv_b.at[slot, way], send_b_sem.at[slot, way], recv_b_sem.at[slot, way], sides[way])

    def copy_c(block, way):
        slot = lax.rem(block, SLOTS)
        return remote(send_c.at[slot, way], recv_c.at[slot, way], send_c_sem.at[slot, way], recv_c_sem.at[slot, way], sides[way])

    def copies_g(block, turn):
        slot = lax.rem(block, HELD)
        kind, copies = (
            (0, ((me, None, right), (me, None, left), (me, None, partner))),
            (3, ((left, first, right), (right, second, left), (left, None, partner), (right, None, partner))),
            (7, ((far, None, partner),)),
        )[turn]
        made = []
        for i, (shard, rows, other) in enumerate(copies, kind):
            place = held.at[slot, shard] if rows is None else held.at[slot, shard, rows]
            made.append(remote(place, place, send_g_sem.at[i, slot], recv_g_sem.at[i, slot], other))
        return made

    def copy_out(block):
        slot = lax.rem(block, HELD)
        return pltpu.make_async_copy(held.at[slot], sums_ref.at[:, block], out_sem.at[slot])

    def copy_late(block):
        slot = lax.rem(block, HELD)
        return pltpu.make_async_copy(held.at[slot, me], late_ref.at[block - early], out_sem.at[slot])

    def on_chip(slot, which, rows):
        return own[slot, core, which, rows].astype(F32) + recv_a[slot, which, rows].astype(F32)

    def stage(after, low, high):
        def run(do):
            @pl.when((step >= after + low) & (step < after + high))
            def _():
                do(step - after)

        return run

    @pl.when(step == 0)
    def _():
        barrier = pltpu.get_barrier_semaphore()
        for other in (partner, *sides):
            pl.semaphore_signal(barrier, inc=1, device_id={"dp": other}, device_id_type=MESH)

    @pl.when(step == 1)
    def _():
        pl.semaphore_wait(pltpu.get_barrier_semaphore(), 3)

    @stage(8, 0, early)
    def _(block):
        copy_out(block).wait()

    @stage(7, 0, early)
    def _(block):
        for copy in copies_g(block, 2):
            copy.wait()
        copy_out(block).start()

    @stage(6, 0, early)
    def _(block):
        for copy in copies_g(block, 1):
            copy.wait()
        for copy in copies_g(block, 2):
            copy.start()

    @stage(5, 0, early)
    def _(block):
        for copy in copies_g(block, 0):
            copy.wait()
        for copy in copies_g(block, 1):
            copy.start()

    @stage(5, early, blocks)
    def _(block):
        copy_late(block).wait()

    @stage(4, 0, blocks)
    def _(block):
        slot = lax.rem(block, SLOTS)
        copy_c(block, 0).wait()
        copy_c(block, 1).wait()
        for rows in (first, second):
            total = on_chip(slot, chip, rows) + recv_c[slot, 0, rows].astype(F32) + recv_c[slot, 1, rows].astype(F32)
            held[lax.rem(block, HELD), me, rows] = total.astype(BF16)

    @stage(3, 0, blocks)
    def _(block):
        slot = lax.rem(block, SLOTS)
        copy_b(block, 0).wait()
        copy_b(block, 1).wait()
        send_c[slot, 0, first] = (on_chip(slot, right_chip, first) + recv_b[slot, 0].astype(F32)).astype(BF16)
        send_c[slot, 0, second] = on_chip(slot, right_chip, second).astype(BF16)
        send_c[slot, 1, first] = on_chip(slot, left_chip, first).astype(BF16)
        send_c[slot, 1, second] = (on_chip(slot, left_chip, second) + recv_b[slot, 1].astype(F32)).astype(BF16)
        copy_c(block, 0).start()
        copy_c(block, 1).start()

    @stage(2, 0, blocks)
    def _(block):
        slot = lax.rem(block, SLOTS)
        copy_a(block).wait()
        send_b[slot, 0] = on_chip(slot, far_chip, first).astype(BF16)
        send_b[slot, 1] = on_chip(slot, far_chip, second).astype(BF16)
        copy_b(block, 0).start()
        copy_b(block, 1).start()

    @stage(1, 0, blocks)
    def _(block):
        copy_a(block).start()

    @stage(4, 0, early)
    def _(block):
        for copy in copies_g(block, 0):
            copy.start()

    @stage(4, early, blocks)
    def _(block):
        copy_late(block).start()

    eye = (lax.broadcasted_iota(jnp.int32, (FB, FB), 0) == lax.broadcasted_iota(jnp.int32, (FB, FB), 1)).astype(BF16)

    for number in range(layers):

        @pl.when(step == (layers - 1 - number) * each)
        def _(number=number):
            def tile(i, _):
                rows = pl.ds(pl.multiple_of(i * TT, TT), TT)
                if number == layers - 1:
                    g_ref[rows, :] = dy_ref[rows, :]
                else:
                    wide = kept[number + 1][rows, :].astype(F32)
                    scale = scale_of(wide)
                    da = acc_ref[rows, :].astype(BF16).astype(F32)
                    along = jnp.mean(da * wide, -1, keepdims=True)
                    dwide = (da * scale - wide * (scale * scale * scale * along)).astype(BF16)
                    g_ref[rows, :] = (g_ref[rows, :].astype(F32) + dwide.astype(F32)).astype(BF16)
                if number:
                    acc_ref[rows, :] = jnp.zeros((TT, d), F32)
                wide = kept[number][rows, :].astype(F32)
                a_ref[rows, :] = (wide * scale_of(wide)).astype(BF16)
                for j in range(d // FB):
                    at_ref[j * FB : (j + 1) * FB, rows] = transposed(eye, a_ref[rows, j * FB : (j + 1) * FB])
                    gt_ref[j * FB : (j + 1) * FB, rows] = transposed(eye, g_ref[rows, j * FB : (j + 1) * FB])
                return 0

            lax.fori_loop(0, tokens // TT, tile, 0)

    @stage(0, 0, blocks)
    def _(block):
        slot = lax.rem(block, SLOTS)
        wg, wu, wd = wg_ref[0], wu_ref[0], wd_ref[0]
        for i in range(tokens // TT):
            rows = pl.ds(i * TT, TT)
            a = a_ref[rows, :]
            gate, up = dot(a, wg), dot(a, wu)
            dhid = dot_nt(g_ref[rows, :], wd).astype(BF16).astype(F32)
            sig = sigmoid(gate)
            silu = gate * sig
            hid_ref[rows, :] = (silu * up).astype(BF16)
            dup_ref[rows, :] = (dhid * silu).astype(BF16)
            dgate_ref[rows, :] = (dhid * up * (sig + silu * (1.0 - sig))).astype(BF16)
        part, down = d // n, FB // n
        for i in range(d // FB):
            rows = pl.ds(i * FB, FB)
            dwg = dot(at_ref[rows, :], dgate_ref[...]).astype(BF16)
            dwu = dot(at_ref[rows, :], dup_ref[...]).astype(BF16)
            dwd = transposed(eye, dot(gt_ref[rows, :], hid_ref[...]).astype(BF16))
            lo, hi = i * FB, (i + 1) * FB
            for k in range(n):
                top, end = max(lo, k * part), min(hi, (k + 1) * part)
                if top < end:
                    own[slot, k % 2, k // 2, top - k * part : end - k * part, :] = dwg[top - lo : end - lo]
                    own[slot, k % 2, k // 2, part + top - k * part : part + end - k * part, :] = dwu[top - lo : end - lo]
                own[slot, k % 2, k // 2, 2 * part + i * down : 2 * part + (i + 1) * down, :] = dwd[k * down : (k + 1) * down]

    @stage(0, 0, blocks - each)
    def _(block):
        for i in range(tokens // TT):
            rows = pl.ds(i * TT, TT)
            acc_ref[rows, :] += dot_nt(dgate_ref[rows, :], wg_ref[0]) + dot_nt(dup_ref[rows, :], wu_ref[0])


def backward(kept, dy, weights, n, late):
    tokens, d = dy.shape
    layers, _, ff = weights[0].shape
    each = ff // FB
    blocks = layers * each
    chips, share = n // 2, 3 * d // n
    assert chips == 4 and 3 < late <= each
    whole = pl.BlockSpec((tokens, d), lambda s: (0, 0), pipeline_mode=pl.Buffered(1))

    def at(s):
        s = jnp.minimum(s, blocks - 1)
        return layers - 1 - lax.div(s, each), lax.rem(s, each)

    def wide_at(s):
        number, f = at(s)
        return number, 0, f

    def tall_at(s):
        number, f = at(s)
        return number, f, 0

    def vmem(*shape):
        return pltpu.VMEM(shape, BF16)

    scratch = [vmem(tokens, d), vmem(tokens, d), vmem(d, tokens), vmem(d, tokens)]
    scratch += [vmem(tokens, FB)] * 3 + [pltpu.VMEM((tokens, d), F32)]
    scratch += [vmem(SLOTS, 2, chips, share, FB), vmem(SLOTS, chips, share, FB)]
    scratch += [vmem(SLOTS, 2, share // 2, FB)] * 2 + [vmem(SLOTS, 2, share, FB)] * 2 + [vmem(HELD, n, share, FB)]
    scratch += [pltpu.SemaphoreType.DMA((SLOTS,))] * 2 + [pltpu.SemaphoreType.DMA((SLOTS, 2))] * 4
    scratch += [pltpu.SemaphoreType.DMA((8, HELD))] * 2 + [pltpu.SemaphoreType.DMA((HELD,))]
    return pl.pallas_call(
        functools.partial(backward_kernel, n, layers, late),
        grid=(blocks + SLOTS + 1,),
        in_specs=[whole] * (layers + 1)
        + [pl.BlockSpec((1, d, FB), wide_at), pl.BlockSpec((1, d, FB), wide_at), pl.BlockSpec((1, FB, d), tall_at)],
        out_specs=[pl.BlockSpec(memory_space=pl.ANY)] * 2,
        out_shape=[
            jax.ShapeDtypeStruct((n, blocks - late, share, FB), BF16),
            jax.ShapeDtypeStruct((late, share, FB), BF16),
        ],
        scratch_shapes=scratch,
        compiler_params=pltpu.CompilerParams(
            vmem_limit_bytes=VMEM, dimension_semantics=("arbitrary",), collective_id=0, has_side_effects=True
        ),
        cost_estimate=pl.CostEstimate(
            flops=(16 * layers - 4) * tokens * d * ff, bytes_accessed=6 * tokens * d + 12 * layers * d * ff, transcendentals=layers * tokens * ff
        ),
        name="backward",
    )(*kept, dy, *weights)


def adamw_kernel(sum_ref, *refs):
    ws, ms, vs, outs = refs[:3], refs[3:6], refs[6:9], refs[-9:]
    share = sum_ref.shape[2] // 3
    some = sum_ref.shape[0]
    for i in range(3):
        if i < 2:
            g = sum_ref[:, 0, i * share : (i + 1) * share, :].reshape(some * share, FB)
        else:
            down = ws[2].shape[1] // some
            pieces = [
                sum_ref[:, 0, 2 * share + j * down : 2 * share + (j + 1) * down, :].reshape(some * down, FB) for j in range(share // down)
            ]
            g = jnp.concatenate(pieces, axis=1)
        g = g.astype(F32)
        w, m, v = ws[i][0].astype(F32), ms[i][0], vs[i][0]
        m = 0.9 * m + 0.1 * g
        v = 0.95 * v + 0.05 * g * g
        step = m * lax.rsqrt(v + 1e-8) + 0.1 * w
        outs[i][0] = (w - 0.02 * step).astype(BF16)
        outs[3 + i][0] = m
        outs[6 + i][0] = v


def adamw(sums, arrays, number, blocks, offset, so_far):
    n, _, share, _ = sums.shape
    d = arrays[0].shape[1]
    parts = 2
    low, high = blocks
    wide = pl.BlockSpec((1, d // parts, FB), lambda f, p: (number, p, low + f))
    tall = pl.BlockSpec((1, FB // parts, d), lambda f, p: (number, (low + f) * parts + p, 0))
    three = [wide, wide, tall]
    held = list(so_far) if so_far is not None else []
    size = 3 * d * FB * (high - low)
    return pl.pallas_call(
        adamw_kernel,
        grid=(high - low, parts),
        in_specs=[pl.BlockSpec((n // parts, 1, share, FB), lambda f, p: (p, offset + f, 0, 0))]
        + three * 3
        + [pl.BlockSpec(memory_space=pl.ANY)] * len(held),
        out_specs=three * 3,
        out_shape=[jax.ShapeDtypeStruct(a.shape, a.dtype) for a in arrays],
        input_output_aliases={10 + i: i for i in range(len(held))},
        compiler_params=pltpu.CompilerParams(vmem_limit_bytes=VMEM, dimension_semantics=("arbitrary", "arbitrary")),
        cost_estimate=pl.CostEstimate(flops=14 * size, bytes_accessed=22 * size, transcendentals=size),
        name=f"adamw_{number}_{low}",
    )(sums, *arrays, *held)


def solution(mesh):
    n = mesh.shape["dp"]

    def step(x, dy, *arrays):
        weights = arrays[:3]
        layers, _, ff = weights[0].shape
        each = ff // FB
        kept = [x[0]]
        for number in range(layers - 1):
            kept.append(forward(kept[-1], weights, number))
        sums, shards = backward(kept, dy[0], weights, n, LATE)
        late = lax.all_gather(shards, "dp")
        new = None
        for number in reversed(range(layers)):
            high = each if number else each - LATE
            if high:
                new = adamw(sums, arrays, number, (0, high), (layers - 1 - number) * each, new)
        return tuple(adamw(late, arrays, 0, (each - LATE, each), 0, new))

    return jax.shard_map(
        step,
        mesh=mesh,
        in_specs=(P(("rep", "dp"), None, None),) * 2 + (P(None, None, None),) * 9,
        out_specs=(P("rep", None, None),) * 9,
        check_vma=False,
    )
```

```python
import functools

import jax
import jax.numpy as jnp
from jax import lax
from jax.experimental import pallas as pl
from jax.experimental.pallas import tpu as pltpu
from jax.sharding import PartitionSpec as P

BF16, F32 = jnp.bfloat16, jnp.float32
FB = 256
FB_FWD = 256
TT, TT_FWD = 512, 1024
VMEM = 60 * 2**20


def dot(a, b):
    return jnp.dot(a, b, preferred_element_type=F32)


def dot_nt(a, b):
    return lax.dot_general(a, b, (((1,), (1,)), ((), ())), preferred_element_type=F32)


def transposed(eye, x):
    return dot_nt(eye, x).astype(BF16)


def scale_of(wide):
    return lax.rsqrt(jnp.mean(wide * wide, -1, keepdims=True) + 1e-6)


def sigmoid(x):
    return 1.0 / (1.0 + jnp.exp(-x))


def forward_kernel(h_ref, wg_ref, wu_ref, wd_ref, out_ref, hid_ref):
    wide = h_ref[...].astype(F32)
    a = (wide * scale_of(wide)).astype(BF16)
    for f in range(0, hid_ref.shape[1], FB_FWD):
        units = pl.ds(f, FB_FWD)
        gate, up = dot(a, wg_ref[0, :, units]), dot(a, wu_ref[0, :, units])
        hid_ref[:, units] = (gate * sigmoid(gate) * up).astype(BF16)
    down = dot(hid_ref[...], wd_ref[0]).astype(BF16).astype(F32)
    out_ref[...] = (h_ref[...].astype(F32) + down).astype(BF16)


def forward(h, weights, number):
    tokens, d = h.shape
    ff = weights[0].shape[2]
    tile = pl.BlockSpec((TT_FWD, d), lambda t: (t, 0))
    return pl.pallas_call(
        forward_kernel,
        grid=(tokens // TT_FWD,),
        in_specs=[tile] + [pl.BlockSpec((1, *w.shape[1:]), lambda t: (number, 0, 0), pipeline_mode=pl.Buffered(1)) for w in weights],
        out_specs=tile,
        out_shape=jax.ShapeDtypeStruct((tokens, d), BF16),
        scratch_shapes=[pltpu.VMEM((TT_FWD, ff), BF16)],
        compiler_params=pltpu.CompilerParams(vmem_limit_bytes=VMEM, dimension_semantics=("arbitrary",)),
        cost_estimate=pl.CostEstimate(flops=6 * tokens * d * ff, bytes_accessed=4 * tokens * d + 6 * d * ff, transcendentals=tokens * ff),
        name="layer_forward",
    )(h, *weights)


SLOTS, HELD = 4, 8
LATE = 7
MESH = pl.DeviceIdType.MESH


def backward_kernel(n, layers, late, *refs):
    kept, (dy_ref, wg_ref, wu_ref, wd_ref, sums_ref, late_ref), refs = refs[:layers], refs[layers : layers + 6], refs[layers + 6 :]
    g_ref, a_ref, at_ref, gt_ref, hid_ref, dgate_ref, dup_ref, acc_ref, *refs = refs
    own, recv_a, send_b, recv_b, send_c, recv_c, held, *sems = refs
    send_a_sem, recv_a_sem, send_b_sem, recv_b_sem, send_c_sem, recv_c_sem, send_g_sem, recv_g_sem, out_sem = sems
    step = pl.program_id(0)
    tokens, d = dy_ref.shape
    blocks = pl.num_programs(0) - SLOTS - 1
    each, early = blocks // layers, blocks - late
    share, half = own.shape[3], own.shape[3] // 2
    chips = n // 2
    me = lax.axis_index("dp")
    chip, core = lax.div(me, 2), lax.rem(me, 2)
    right_chip, far_chip, left_chip = (lax.rem(chip + i, chips) for i in (1, 2, 3))
    partner = chip * 2 + (1 - core)
    right, far, left = (c * 2 + core for c in (right_chip, far_chip, left_chip))
    sides = (right, left)
    first, second = pl.ds(0, half), pl.ds(half, half)

    def remote(src, dst, send, recv, other):
        return pltpu.make_async_remote_copy(src, dst, send, recv, device_id={"dp": other}, device_id_type=MESH)

    def copy_a(block):
        slot = lax.rem(block, SLOTS)
        return remote(own.at[slot, 1 - core], recv_a.at[slot], send_a_sem.at[slot], recv_a_sem.at[slot], partner)

    def copy_b(block, way):
        slot = lax.rem(block, SLOTS)
        return remote(send_b.at[slot, way], recv_b.at[slot, way], send_b_sem.at[slot, way], recv_b_sem.at[slot, way], sides[way])

    def copy_c(block, way):
        slot = lax.rem(block, SLOTS)
        return remote(send_c.at[slot, way], recv_c.at[slot, way], send_c_sem.at[slot, way], recv_c_sem.at[slot, way], sides[way])

    def copies_g(block, turn):
        slot = lax.rem(block, HELD)
        kind, copies = (
            (0, ((me, None, right), (me, None, left), (me, None, partner))),
            (3, ((left, first, right), (right, second, left), (left, None, partner), (right, None, partner))),
            (7, ((far, None, partner),)),
        )[turn]
        made = []
        for i, (shard, rows, other) in enumerate(copies, kind):
            place = held.at[slot, shard] if rows is None else held.at[slot, shard, rows]
            made.append(remote(place, place, send_g_sem.at[i, slot], recv_g_sem.at[i, slot], other))
        return made

    def copy_out(block):
        slot = lax.rem(block, HELD)
        return pltpu.make_async_copy(held.at[slot], sums_ref.at[:, block], out_sem.at[slot])

    def copy_late(block):
        slot = lax.rem(block, HELD)
        return pltpu.make_async_copy(held.at[slot, me], late_ref.at[block - early], out_sem.at[slot])

    def on_chip(slot, which, rows):
        return own[slot, core, which, rows].astype(F32) + recv_a[slot, which, rows].astype(F32)

    def stage(after, low, high):
        def run(do):
            @pl.when((step >= after + low) & (step < after + high))
            def _():
                do(step - after)

        return run

    @pl.when(step == 0)
    def _():
        barrier = pltpu.get_barrier_semaphore()
        for other in (partner, *sides):
            pl.semaphore_signal(barrier, inc=1, device_id={"dp": other}, device_id_type=MESH)

    @pl.when(step == 1)
    def _():
        pl.semaphore_wait(pltpu.get_barrier_semaphore(), 3)

    @stage(10, 0, early)
    def _(block):
        copy_out(block).wait()

    @stage(9, 0, early)
    def _(block):
        for copy in copies_g(block, 2):
            copy.wait()
        copy_out(block).start()

    @stage(5, early, blocks)
    def _(block):
        copy_late(block).wait()

    @stage(4, 0, blocks)
    def _(block):
        slot = lax.rem(block, SLOTS)
        copy_c(block, 0).wait()
        copy_c(block, 1).wait()
        for rows in (first, second):
            total = on_chip(slot, chip, rows) + recv_c[slot, 0, rows].astype(F32) + recv_c[slot, 1, rows].astype(F32)
            held[lax.rem(block, HELD), me, rows] = total.astype(BF16)

    @stage(3, 0, blocks)
    def _(block):
        slot = lax.rem(block, SLOTS)
        copy_b(block, 0).wait()
        copy_b(block, 1).wait()
        send_c[slot, 0, first] = (on_chip(slot, right_chip, first) + recv_b[slot, 0].astype(F32)).astype(BF16)
        send_c[slot, 0, second] = on_chip(slot, right_chip, second).astype(BF16)
        send_c[slot, 1, first] = on_chip(slot, left_chip, first).astype(BF16)
        send_c[slot, 1, second] = (on_chip(slot, left_chip, second) + recv_b[slot, 1].astype(F32)).astype(BF16)
        copy_c(block, 0).start()
        copy_c(block, 1).start()

    @stage(2, 0, blocks)
    def _(block):
        slot = lax.rem(block, SLOTS)
        copy_a(block).wait()
        send_b[slot, 0] = on_chip(slot, far_chip, first).astype(BF16)
        send_b[slot, 1] = on_chip(slot, far_chip, second).astype(BF16)
        copy_b(block, 0).start()
        copy_b(block, 1).start()

    @stage(1, 0, blocks)
    def _(block):
        copy_a(block).start()

    @stage(8, 0, early)
    def _(block):
        for copy in copies_g(block, 1):
            copy.wait()
        for copy in copies_g(block, 2):
            copy.start()

    @stage(6, 0, early)
    def _(block):
        for copy in copies_g(block, 0):
            copy.wait()
        for copy in copies_g(block, 1):
            copy.start()

    @stage(4, 0, early)
    def _(block):
        for copy in copies_g(block, 0):
            copy.start()

    @stage(4, early, blocks)
    def _(block):
        copy_late(block).start()

    eye = (lax.broadcasted_iota(jnp.int32, (FB, FB), 0) == lax.broadcasted_iota(jnp.int32, (FB, FB), 1)).astype(BF16)

    for number in range(layers):

        @pl.when(step == (layers - 1 - number) * each)
        def _(number=number):
            def tile(i, _):
                rows = pl.ds(pl.multiple_of(i * TT, TT), TT)
                if number == layers - 1:
                    g_ref[rows, :] = dy_ref[rows, :]
                else:
                    wide = kept[number + 1][rows, :].astype(F32)
                    scale = scale_of(wide)
                    da = acc_ref[rows, :].astype(BF16).astype(F32)
                    along = jnp.mean(da * wide, -1, keepdims=True)
                    dwide = (da * scale - wide * (scale * scale * scale * along)).astype(BF16)
                    g_ref[rows, :] = (g_ref[rows, :].astype(F32) + dwide.astype(F32)).astype(BF16)
                if number:
                    acc_ref[rows, :] = jnp.zeros((TT, d), F32)
                wide = kept[number][rows, :].astype(F32)
                a_ref[rows, :] = (wide * scale_of(wide)).astype(BF16)
                for j in range(d // FB):
                    at_ref[j * FB : (j + 1) * FB, rows] = transposed(eye, a_ref[rows, j * FB : (j + 1) * FB])
                    gt_ref[j * FB : (j + 1) * FB, rows] = transposed(eye, g_ref[rows, j * FB : (j + 1) * FB])
                return 0

            lax.fori_loop(0, tokens // TT, tile, 0)

    @stage(0, 0, blocks)
    def _(block):
        slot = lax.rem(block, SLOTS)
        wg, wu, wd = wg_ref[0], wu_ref[0], wd_ref[0]
        for i in range(tokens // TT):
            rows = pl.ds(i * TT, TT)
            a = a_ref[rows, :]
            gate, up = dot(a, wg), dot(a, wu)
            dhid = dot_nt(g_ref[rows, :], wd).astype(BF16).astype(F32)
            sig = sigmoid(gate)
            silu = gate * sig
            hid_ref[rows, :] = (silu * up).astype(BF16)
            dup_ref[rows, :] = (dhid * silu).astype(BF16)
            dgate_ref[rows, :] = (dhid * up * (sig + silu * (1.0 - sig))).astype(BF16)
        part, down = d // n, FB // n
        for i in range(d // FB):
            rows = pl.ds(i * FB, FB)
            dwd = dot(gt_ref[rows, :], hid_ref[...]).astype(BF16)
            dwg = dot(at_ref[rows, :], dgate_ref[...]).astype(BF16)
            dwu = dot(at_ref[rows, :], dup_ref[...]).astype(BF16)
            dwd = dwd.T
            lo, hi = i * FB, (i + 1) * FB
            for k in range(n):
                top, end = max(lo, k * part), min(hi, (k + 1) * part)
                if top < end:
                    own[slot, k % 2, k // 2, top - k * part : end - k * part, :] = dwg[top - lo : end - lo]
                    own[slot, k % 2, k // 2, part + top - k * part : part + end - k * part, :] = dwu[top - lo : end - lo]
                own[slot, k % 2, k // 2, 2 * part + i * down : 2 * part + (i + 1) * down, :] = dwd[k * down : (k + 1) * down]

    @stage(0, 0, blocks - each)
    def _(block):
        for i in range(tokens // TT):
            rows = pl.ds(i * TT, TT)
            acc_ref[rows, :] += dot_nt(dgate_ref[rows, :], wg_ref[0]) + dot_nt(dup_ref[rows, :], wu_ref[0])


def backward(kept, dy, weights, n, late):
    tokens, d = dy.shape
    layers, _, ff = weights[0].shape
    each = ff // FB
    blocks = layers * each
    chips, share = n // 2, 3 * d // n
    assert chips == 4 and 5 < late <= each
    whole = pl.BlockSpec((tokens, d), lambda s: (0, 0), pipeline_mode=pl.Buffered(1))

    def at(s):
        s = jnp.minimum(s, blocks - 1)
        return layers - 1 - lax.div(s, each), lax.rem(s, each)

    def wide_at(s):
        number, f = at(s)
        return number, 0, f

    def tall_at(s):
        number, f = at(s)
        return number, f, 0

    def vmem(*shape):
        return pltpu.VMEM(shape, BF16)

    scratch = [vmem(tokens, d), vmem(tokens, d), vmem(d, tokens), vmem(d, tokens)]
    scratch += [vmem(tokens, FB)] * 3 + [pltpu.VMEM((tokens, d), F32)]
    scratch += [vmem(SLOTS, 2, chips, share, FB), vmem(SLOTS, chips, share, FB)]
    scratch += [vmem(SLOTS, 2, share // 2, FB)] * 2 + [vmem(SLOTS, 2, share, FB)] * 2 + [vmem(HELD, n, share, FB)]
    scratch += [pltpu.SemaphoreType.DMA((SLOTS,))] * 2 + [pltpu.SemaphoreType.DMA((SLOTS, 2))] * 4
    scratch += [pltpu.SemaphoreType.DMA((8, HELD))] * 2 + [pltpu.SemaphoreType.DMA((HELD,))]
    return pl.pallas_call(
        functools.partial(backward_kernel, n, layers, late),
        grid=(blocks + SLOTS + 1,),
        in_specs=[whole] * (layers + 1)
        + [pl.BlockSpec((1, d, FB), wide_at), pl.BlockSpec((1, d, FB), wide_at), pl.BlockSpec((1, FB, d), tall_at)],
        out_specs=[pl.BlockSpec(memory_space=pl.ANY)] * 2,
        out_shape=[
            jax.ShapeDtypeStruct((n, blocks - late, share, FB), BF16),
            jax.ShapeDtypeStruct((late, share, FB), BF16),
        ],
        scratch_shapes=scratch,
        compiler_params=pltpu.CompilerParams(
            vmem_limit_bytes=VMEM, dimension_semantics=("arbitrary",), collective_id=0, has_side_effects=True
        ),
        cost_estimate=pl.CostEstimate(
            flops=(16 * layers - 4) * tokens * d * ff, bytes_accessed=6 * tokens * d + 12 * layers * d * ff, transcendentals=layers * tokens * ff
        ),
        name="backward",
    )(*kept, dy, *weights)


def adamw_kernel(sum_ref, *refs):
    ws, ms, vs, outs = refs[:3], refs[3:6], refs[6:9], refs[-9:]
    share = sum_ref.shape[2] // 3
    some = sum_ref.shape[0]
    for i in range(3):
        if i < 2:
            g = sum_ref[:, 0, i * share : (i + 1) * share, :].reshape(some * share, FB)
        else:
            down = ws[2].shape[1] // some
            pieces = [
                sum_ref[:, 0, 2 * share + j * down : 2 * share + (j + 1) * down, :].reshape(some * down, FB) for j in range(share // down)
            ]
            g = jnp.concatenate(pieces, axis=1)
        g = g.astype(F32)
        w, m, v = ws[i][0].astype(F32), ms[i][0], vs[i][0]
        m = 0.9 * m + 0.1 * g
        v = 0.95 * v + 0.05 * g * g
        step = m * lax.rsqrt(v + 1e-8) + 0.1 * w
        outs[i][0] = (w - 0.02 * step).astype(BF16)
        outs[3 + i][0] = m
        outs[6 + i][0] = v


def adamw(sums, arrays, first, last, so_far):
    n, _, share, _ = sums.shape
    layers, d, ff = arrays[0].shape
    each = ff // FB

    def at(f):
        return layers - 1 - lax.div(first + f, each), lax.rem(first + f, each)

    def wide_at(f):
        number, block = at(f)
        return number, 0, block

    def tall_at(f):
        number, block = at(f)
        return number, block, 0

    wide, tall = pl.BlockSpec((1, d, FB), wide_at), pl.BlockSpec((1, FB, d), tall_at)
    three = [wide, wide, tall]
    held = list(so_far) if so_far is not None else []
    size = 3 * d * FB * (last - first)
    return pl.pallas_call(
        adamw_kernel,
        grid=(last - first,),
        in_specs=[pl.BlockSpec((n, 1, share, FB), lambda f: (0, f, 0, 0))] + three * 3 + [pl.BlockSpec(memory_space=pl.ANY)] * len(held),
        out_specs=three * 3,
        out_shape=[jax.ShapeDtypeStruct(a.shape, a.dtype) for a in arrays],
        input_output_aliases={10 + i: i for i in range(len(held))},
        compiler_params=pltpu.CompilerParams(vmem_limit_bytes=VMEM, dimension_semantics=("arbitrary",)),
        cost_estimate=pl.CostEstimate(flops=14 * size, bytes_accessed=22 * size, transcendentals=size),
        name=f"adamw_{first}",
    )(sums, *arrays, *held)


def solution(mesh):
    n = mesh.shape["dp"]

    def step(x, dy, *arrays):
        weights = arrays[:3]
        layers, _, ff = weights[0].shape
        kept = [x[0]]
        for number in range(layers - 1):
            kept.append(forward(kept[-1], weights, number))
        sums, shards = backward(kept, dy[0], weights, n, LATE)
        late = lax.all_gather(shards, "dp")
        blocks = layers * (ff // FB)
        new = adamw(sums, arrays, 0, blocks - LATE, None)
        return tuple(adamw(late, arrays, blocks - LATE, blocks, new))

    return jax.shard_map(
        step,
        mesh=mesh,
        in_specs=(P(("rep", "dp"), None, None),) * 2 + (P(None, None, None),) * 9,
        out_specs=(P("rep", None, None),) * 9,
        check_vma=False,
    )
```
